32 devices in a mesh: groups: 2 (over y), gx: 4 (over z), gy: 4 (over x, core).
Axes of the slice: x: 2, y: 2, z: 4, core: 2. Of those that a mesh axis runs over, the one named last changes fastest.
Arguments:
- tokens: bfloat16 [2, 16, 16384], P(None, 'groups', 'gx'), parts along dimension 1, may hold values from -20 to 20, as said below
- lengths: int32 [2, 16], P(None, ('groups', 'gx')), parts along dimension 1, may hold values from 1 to 1024, as said below
- norm_gain: bfloat16 [16384], P('gx'), may hold values from 0.5 to 2
- w_query: bfloat16 [16384, 8192], P('gx', 'gy'), may hold values from -1.171875 to 1.171875
- key_value_weight: bfloat16 [16384, 4, 256], P('gx', 'gy'), may hold values from -0.046875 to 0.046875
- w_out: bfloat16 [8192, 16384], P('gy', 'gx'), may hold values from -0.0625 to 0.0625
- cache: bfloat16 [2, 16, 1024, 4, 2, 128], P(None, ('groups', 'gx'), None, 'gy'), parts along dimension 1, may hold values from -16 to 16
Outputs:
- layer_out: bfloat16 [2, 16, 16384], P(None, 'groups', 'gx'), parts along dimension 1
The draws below stay inside these ranges and needn't reach their ends.
There are 2 independent parts, one for each index of `groups`. The reference program is written for one: setup_inputs(seed, part) draws one part's arguments, and reference() takes and returns one part's arrays. A program takes and returns all parts, laid end to end along the dimension named above; an argument that names none is the same for every part. Nothing has to cross between parts.
Inputs may be any that keep to these rules, and one draw needn't show every extreme that they name: `tokens`: entries vary with the feature and the row. `lengths`: some rollout has exactly 1024 cached positions in every draw.
All inputs are finite; a program needn't handle non-finite values.
Results may differ from the reference program's by a relative error of at most 0.012.
The reference program's roundings to bfloat16 on the way count: a program that leaves them out, or rounds other values in their place, can miss the bound.
Values may be sent and summed in bfloat16 or wider, within the bound.
A program may use at most 128 MiB of HBM per device.

```python
import math
import jax
import jax.numpy as jnp
from jax import lax

MODEL_WIDTH = 16384
QUERY_HEADS = 64
KEY_VALUE_HEADS = 4
HEAD_SIZE = 128
MICRO_BATCHES = 2
CACHE_POSITIONS = 1024
BATCH_ROLLOUTS = 8


def draw_tokens(key, part):
    first = jax.random.fold_in(key, 0)
    columns = jnp.exp(jnp.linspace(jnp.log(0.5), jnp.log(1.5), MODEL_WIDTH)).astype(jnp.float32)
    base = jax.random.truncated_normal(first, -6.0, 6.0, (MICRO_BATCHES, BATCH_ROLLOUTS, MODEL_WIDTH), jnp.float32)
    return (base * columns).astype(jnp.bfloat16)


def draw_lengths(key, part):
    counts = jax.random.randint(key, (MICRO_BATCHES, BATCH_ROLLOUTS), 1, CACHE_POSITIONS + 1, dtype=jnp.int32)
    return counts.at[0, 0].set(CACHE_POSITIONS)


def draw_w_query(key, part):
    first = jax.random.fold_in(jax.random.fold_in(key, 7), 0)
    base = jax.random.truncated_normal(first, -6.0, 6.0, (MODEL_WIDTH, QUERY_HEADS * HEAD_SIZE), jnp.float32) * MODEL_WIDTH ** (-0.5)
    return base.astype(jnp.bfloat16)


def draw_cache(key, part):
    factor = jnp.array([2.5, 1.0], dtype=jnp.float32).reshape(1, 1, 1, 1, 2, 1)
    array_shape = (MICRO_BATCHES, BATCH_ROLLOUTS, CACHE_POSITIONS, KEY_VALUE_HEADS, 2, HEAD_SIZE)
    base = jax.random.truncated_normal(key, -6.0, 6.0, array_shape, jnp.float32)
    return (base * factor).astype(jnp.bfloat16)


def block_levels(key, extent, cuts, low, largest):
    gain, own = 1.0, jax.random.fold_in(key, 6)
    for dim, shards_of in cuts:
        draws = jnp.exp(jax.random.uniform(jax.random.fold_in(own, dim), (shards_of,), jnp.float32, low / len(cuts), largest / len(cuts)))
        gain = gain * jnp.repeat(draws, extent[dim] // shards_of).reshape([-1 if axis == dim else 1 for axis in range(len(extent))])
    return gain


def scatter_about(own_key, shape, width, reach, cuts=(), held_as=jnp.bfloat16):
    drawn = jax.random.normal(own_key, shape, jnp.float32) * width
    if len(cuts) > 0:
        drawn = block_levels(own_key, shape, cuts, -0.22, 0.18) * drawn
    return jnp.clip(drawn, min=-reach, max=reach).astype(held_as)


def setup_inputs(seed: int = 0, part: int = 0) -> dict:
    arg_keys = jax.random.split(jax.random.key(seed), 8)
    own_keys = jax.random.split(jax.random.fold_in(arg_keys[7], part), 8)
    return {
        "tokens": draw_tokens(jax.random.fold_in(jax.random.fold_in(arg_keys[7], part), 71), part),
        "lengths": draw_lengths(jax.random.fold_in(jax.random.fold_in(arg_keys[7], part), 71), part),
        "norm_gain": jnp.clip(jnp.exp(math.log(2.0) - 1.3862944 * jax.random.uniform(arg_keys[2], (MODEL_WIDTH,), jnp.float32) ** block_levels(arg_keys[2], (MODEL_WIDTH,), ((0, 4),), -0.2, 0.2)), 0.5, 2.0).astype(jnp.bfloat16),
        "w_query": draw_w_query(jax.random.fold_in(arg_keys[7], 71), part),
        "key_value_weight": scatter_about(arg_keys[4], (MODEL_WIDTH, KEY_VALUE_HEADS, 2 * HEAD_SIZE), MODEL_WIDTH ** -0.5, 0.046875, ((0, 4), (1, 4))),
        "w_out": scatter_about(arg_keys[5], (QUERY_HEADS * HEAD_SIZE, MODEL_WIDTH), (QUERY_HEADS * HEAD_SIZE) ** -0.5, 0.0625, ((0, 4), (1, 4))),
        "cache": draw_cache(jax.random.fold_in(jax.random.fold_in(arg_keys[7], part), 71), part),
    }


def rotate(vectors, positions):
    half = vectors.shape[-1] // 2
    freq = 500000.0 ** (-2.0 * jnp.arange(half, dtype=jnp.float32) / vectors.shape[-1])
    angle = positions[..., None] * freq
    cosine = jnp.cos(angle)
    sine = jnp.sin(angle)
    first = vectors[..., :half]
    second = vectors[..., half:]
    return jnp.concatenate([first * cosine - second * sine, second * cosine + first * sine], axis=-1)

def reference(tokens, lengths, norm_gain, w_query, key_value_weight, w_out, cache):
    x_full = tokens.astype(jnp.float32)
    score_scale = lax.rsqrt(lax.optimization_barrier(jnp.mean(x_full * x_full, axis=-1)) + 1e-05)
    normed = (x_full * norm_gain.astype(jnp.float32)).astype(jnp.bfloat16)
    flattened = normed.reshape(MICRO_BATCHES * BATCH_ROLLOUTS, MODEL_WIDTH)
    query = jnp.dot(flattened, w_query, preferred_element_type=jnp.float32).reshape(MICRO_BATCHES, BATCH_ROLLOUTS, QUERY_HEADS, HEAD_SIZE)
    query = query * score_scale[:, :, None, None]
    key_value = jnp.dot(flattened, key_value_weight.reshape(MODEL_WIDTH, KEY_VALUE_HEADS * 2 * HEAD_SIZE), preferred_element_type=jnp.float32)
    key_value = key_value.reshape(MICRO_BATCHES, BATCH_ROLLOUTS, KEY_VALUE_HEADS, 2 * HEAD_SIZE) * score_scale[:, :, None, None]
    positions = lengths.astype(jnp.float32)[:, :, None]
    rotated_query = rotate(query, positions).astype(jnp.bfloat16)
    rkey = rotate(key_value[..., :HEAD_SIZE], positions)
    value_new = key_value[..., HEAD_SIZE:]
    query_group = QUERY_HEADS // KEY_VALUE_HEADS
    group_queries = rotated_query.reshape(MICRO_BATCHES, BATCH_ROLLOUTS, KEY_VALUE_HEADS, query_group, HEAD_SIZE)
    inv_root = 1.0 / jnp.sqrt(jnp.float32(HEAD_SIZE))

    def one_batch(items):
        qpart, kpart, vpart, cpart, lpart = items
        keys = cpart[:, :, :, 0, :].astype(jnp.float32)
        values = cpart[:, :, :, 1, :].astype(jnp.float32)
        qfull = qpart.astype(jnp.float32)
        scores = jnp.einsum('rkgd,rskd->rkgs', qfull, keys, precision=lax.Precision.HIGHEST) * inv_root
        valid = jnp.arange(CACHE_POSITIONS, dtype=jnp.int32)[None, :] < lpart[:, None]
        scores = jnp.where(valid[:, None, None, :], scores, -1e+30)
        new_score = lax.optimization_barrier(jnp.sum(qfull * kpart[:, :, None, :], axis=-1)) * inv_root
        top = jnp.maximum(lax.optimization_barrier(jnp.max(scores, axis=-1)), new_score)
        weights = jnp.exp(scores - top[..., None])
        new_weight = jnp.exp(new_score - top)
        total = lax.optimization_barrier(jnp.sum(weights, axis=-1)) + new_weight
        bweights = weights.astype(jnp.bfloat16).astype(jnp.float32)
        summed = jnp.einsum('rkgs,rskd->rkgd', bweights, values, precision=lax.Precision.HIGHEST)
        summed = summed + new_weight[..., None] * vpart[:, :, None, :]
        return (summed / total[..., None]).astype(jnp.bfloat16)
    attended = lax.map(one_batch, (group_queries, rkey, value_new, cache, lengths))
    attended = attended.reshape(MICRO_BATCHES * BATCH_ROLLOUTS, QUERY_HEADS * HEAD_SIZE)
    projected = jnp.dot(attended, w_out, preferred_element_type=jnp.float32).reshape(MICRO_BATCHES, BATCH_ROLLOUTS, MODEL_WIDTH)
    return (x_full + projected).astype(jnp.bfloat16)
```

```python
import functools

import jax
import jax.numpy as jnp
import numpy as np
from jax import lax
from jax.experimental import pallas as pl
from jax.experimental.pallas import tpu as pltpu
from jax.sharding import PartitionSpec as P

MODEL_WIDTH = 16384
HEAD_SIZE = 128
ROPE_BASE = 500000.0
MESH = pl.DeviceIdType.MESH


def kernel(
    n, ny, q_chunk, o_chunk,
    lens, tok_hbm, gain_hbm, freq_hbm, wq_hbm, wk_hbm, wo_hbm, kv_hbm,
    out,
    tok, gain, freq, wq, wk, wo, kv, normed,
    send, recv, q_s, o_s, att_send, att_recv, x_s, ybuf, r1, s2, r2,
    small_sem, wq_sem, wk_sem, wo_sem, kv_sem,
    qs_sem, qr_sem, as_sem, ar_sem, d_send, d_recv, e_send, e_recv, f_send, f_recv,
):
    batches, rows, depth = tok.shape
    here = rows // n
    total_rows = batches * rows
    q_width = wq.shape[1]
    kv_width = wk.shape[1]
    heads = q_width // HEAD_SIZE
    out_width = wo.shape[1]
    nq = q_width // q_chunk
    no = out_width // o_chunk
    local_rows = batches * here
    positions = kv.shape[0] // local_rows
    half = total_rows // 2
    me = lax.axis_index("gx")
    my = lax.axis_index("gy")
    bit = lax.rem(my, 2)

    smalls = [
        pltpu.make_async_copy(tok_hbm, tok, small_sem.at[0]),
        pltpu.make_async_copy(gain_hbm, gain, small_sem.at[1]),
        pltpu.make_async_copy(freq_hbm, freq, small_sem.at[2]),
    ]
    for copy in smalls:
        copy.start()
    wk_copy = pltpu.make_async_copy(wk_hbm, wk, wk_sem)
    wk_copy.start()

    def wq_copy(c):
        cols = pl.ds(pl.multiple_of(c * q_chunk, q_chunk), q_chunk)
        return pltpu.make_async_copy(wq_hbm.at[:, cols], wq.at[:, cols], wq_sem.at[c])

    def wo_copy(c):
        cols = pl.ds(pl.multiple_of(c * o_chunk, o_chunk), o_chunk)
        return pltpu.make_async_copy(wo_hbm.at[:, cols], wo.at[:, cols], wo_sem.at[c])

    kv_copy = pltpu.make_async_copy(kv_hbm, kv, kv_sem)
    for c in range(nq):
        wq_copy(c).start()
    kv_copy.start()
    for c in range(no):
        wo_copy(c).start()

    barrier = pltpu.get_barrier_semaphore()

    def greet(d, carry):
        pl.semaphore_signal(
            barrier, inc=1, device_id={"gx": lax.rem(me + d, n)}, device_id_type=MESH
        )
        return carry

    lax.fori_loop(1, n, greet, 0)
    bits = ny.bit_length() - 1

    def across(level):
        step = 1 << level
        return my + step - 2 * step * lax.rem(my // step, 2)

    for level in range(bits):
        pl.semaphore_signal(barrier, inc=1, device_id={"gy": across(level)}, device_id_type=MESH)

    for copy in smalls:
        copy.wait()
    x = tok[...].astype(jnp.float32).reshape(total_rows, depth)
    normed[...] = (x * gain[...]).astype(jnp.bfloat16)
    squares = jnp.broadcast_to(jnp.sum(x * x, axis=1, keepdims=True), (total_rows, HEAD_SIZE))

    def put(part, start):
        width = part.shape[1]
        for j in range(n):
            for b in range(batches):
                send[j, b * here:(b + 1) * here, pl.ds(start, width)] = part[
                    b * rows + j * here:b * rows + (j + 1) * here, :
                ]

    def shift(c, d, start, width):
        target = lax.rem(me + d, n)
        cols = pl.ds(start, width)
        return pltpu.make_async_remote_copy(
            src_ref=send.at[target, :, cols],
            dst_ref=recv.at[me, :, cols],
            send_sem=qs_sem.at[c, d],
            recv_sem=qr_sem.at[c, d],
            device_id={"gx": target},
            device_id_type=MESH,
        )

    def arrive(c, d, start, width):
        source = lax.rem(me - d + n, n)
        cols = pl.ds(start, width)
        return pltpu.make_async_remote_copy(
            src_ref=send.at[source, :, cols],
            dst_ref=recv.at[source, :, cols],
            send_sem=qs_sem.at[c, d],
            recv_sem=qr_sem.at[c, d],
            device_id={"gx": source},
            device_id_type=MESH,
        )

    def each(fn):
        def body(d, carry):
            fn(d)
            return carry
        lax.fori_loop(1, n, body, 0)

    wk_copy.wait()
    xn = normed[...]
    put(jnp.dot(xn, wk[...], preferred_element_type=jnp.float32), q_width)
    put(squares, q_width + kv_width)
    pl.semaphore_wait(barrier, n - 1 + bits)
    side = kv_width + HEAD_SIZE
    each(lambda d: shift(nq, d, q_width, side).start())

    def project(c, carry):
        start = pl.multiple_of(c * q_chunk, q_chunk)
        wq_copy(c).wait()
        put(
            jnp.dot(
                normed[...], wq[:, pl.ds(start, q_chunk)], preferred_element_type=jnp.float32
            ),
            start,
        )
        each(lambda d: shift(c, d, start, q_chunk).start())
        return carry

    lax.fori_loop(0, nq, project, 0)

    lane = lax.broadcasted_iota(jnp.int32, (local_rows, HEAD_SIZE), 1)
    row = lax.broadcasted_iota(jnp.int32, (local_rows, HEAD_SIZE), 0)
    place = jnp.zeros((local_rows, HEAD_SIZE), jnp.float32)
    for r in range(local_rows):
        place = jnp.where(row == r, lens[r // here, r % here].astype(jnp.float32), place)
    angle = place * freq[...]
    cosine = jnp.cos(angle)
    sine = jnp.sin(angle)
    sine = jnp.where(lane < HEAD_SIZE // 2, -sine, sine)

    def rotate(v):
        return v * cosine + pltpu.roll(v, HEAD_SIZE // 2, 1) * sine

    def finish(c, start, width):
        each(lambda d: arrive(c, d, start, width).wait_recv())

    def summed(start, width):
        cols = pl.ds(start, width)
        total = send[me, :, cols]

        def add(d, acc):
            return acc + recv[lax.rem(me + d, n), :, cols]

        return lax.fori_loop(1, n, add, total, unroll=n <= 8)

    finish(nq, q_width, side)
    tail = summed(q_width, side)
    scale = lax.rsqrt(tail[:, kv_width:] / MODEL_WIDTH + 1e-05)
    rkey = rotate(tail[:, :HEAD_SIZE] * scale)
    value_new = tail[:, HEAD_SIZE:2 * HEAD_SIZE] * scale

    for c in range(nq):
        finish(c, c * q_chunk, q_chunk)
        block = summed(c * q_chunk, q_chunk)
        for h in range(q_chunk // HEAD_SIZE):
            q_s[:, c * (q_chunk // HEAD_SIZE) + h, :] = rotate(
                block[:, h * HEAD_SIZE:(h + 1) * HEAD_SIZE] * scale
            )

    kv_copy.wait()
    inv_root = np.float32(1.0 / np.sqrt(np.float32(HEAD_SIZE)))
    column = lax.broadcasted_iota(jnp.int32, (heads, positions), 1)
    is_key = lax.rem(column, 2) == 0
    for r in range(local_rows):
        pairs = kv[r * positions:(r + 1) * positions, :]
        rquery = q_s[r].astype(jnp.bfloat16)
        scores = (
            lax.dot_general(
                rquery, pairs, (((1,), (1,)), ((), ())), preferred_element_type=jnp.float32
            )
            * inv_root
        )
        valid = jnp.logical_and(is_key, column < 2 * lens[r // here, r % here])
        scores = jnp.where(valid, scores, -1e30)
        new_score = (
            jnp.sum(rquery.astype(jnp.float32) * rkey[r:r + 1, :], axis=1, keepdims=True)
            * inv_root
        )
        top = jnp.maximum(jnp.max(scores, axis=1, keepdims=True), new_score)
        weights = jnp.exp(scores - top)
        new_weight = jnp.exp(new_score - top)
        total = jnp.sum(weights, axis=1, keepdims=True) + new_weight
        moved = pltpu.roll(weights, 1, 1).astype(jnp.bfloat16)
        mixed = jnp.dot(moved, pairs, preferred_element_type=jnp.float32)
        o_s[r] = (mixed + new_weight * value_new[r:r + 1, :]) / total

    for h in range(heads):
        att_send[:, h * HEAD_SIZE:(h + 1) * HEAD_SIZE] = o_s[:, h, :].astype(jnp.bfloat16)

    def spread(d):
        target = lax.rem(me + d, n)
        return pltpu.make_async_remote_copy(
            src_ref=att_send, dst_ref=att_recv.at[me],
            send_sem=as_sem.at[d], recv_sem=ar_sem.at[d],
            device_id={"gx": target}, device_id_type=MESH,
        )

    def gathered(d):
        source = lax.rem(me - d + n, n)
        return pltpu.make_async_remote_copy(
            src_ref=att_send, dst_ref=att_recv.at[source],
            send_sem=as_sem.at[d], recv_sem=ar_sem.at[d],
            device_id={"gx": source}, device_id_type=MESH,
        )

    each(lambda d: spread(d).start())
    att_recv[me] = att_send[...]
    each(lambda d: gathered(d).wait_recv())
    for j in range(n):
        block = att_recv[j].astype(jnp.float32)
        for b in range(batches):
            x_s[b * rows + j * here:b * rows + (j + 1) * here, :] = block[
                b * here:(b + 1) * here, :
            ]
    normed_att = x_s[...].astype(jnp.bfloat16)

    def cols_of(c):
        return pl.ds(pl.multiple_of(c * o_chunk, o_chunk), o_chunk)

    def halve(c):
        cols = cols_of(c)
        return pltpu.make_async_remote_copy(
            src_ref=ybuf.at[1 - bit, :, cols], dst_ref=r1.at[:, cols],
            send_sem=d_send.at[c], recv_sem=d_recv.at[c],
            device_id={"gy": across(0)}, device_id_type=MESH,
        )

    def exchange(c, level):
        cols = cols_of(c)
        return pltpu.make_async_remote_copy(
            src_ref=s2.at[level - 1, :, cols], dst_ref=r2.at[level - 1, :, cols],
            send_sem=e_send.at[level - 1, c], recv_sem=e_recv.at[level - 1, c],
            device_id={"gy": across(level)}, device_id_type=MESH,
        )

    def share(c):
        cols = cols_of(c)
        return pltpu.make_async_remote_copy(
            src_ref=out.at[bit, :, cols], dst_ref=out.at[bit, :, cols],
            send_sem=f_send.at[c], recv_sem=f_recv.at[c],
            device_id={"gy": across(0)}, device_id_type=MESH,
        )

    def shared(c):
        cols = cols_of(c)
        return pltpu.make_async_remote_copy(
            src_ref=out.at[1 - bit, :, cols], dst_ref=out.at[1 - bit, :, cols],
            send_sem=f_send.at[c], recv_sem=f_recv.at[c],
            device_id={"gy": across(0)}, device_id_type=MESH,
        )

    def multiply(c):
        cols = cols_of(c)
        wo_copy(c).wait()
        y = jnp.dot(normed_att, wo[:, cols], preferred_element_type=jnp.float32)
        ybuf[:, :, cols] = y.reshape(2, half, o_chunk)
        halve(c).start()

    def combine(c):
        cols = cols_of(c)
        halve(c).wait_recv()
        s2[0, :, cols] = ybuf[bit, :, cols] + r1[:, cols]
        exchange(c, 1).start()

    def between(c, level):
        cols = cols_of(c)
        exchange(c, level).wait_recv()
        s2[level, :, cols] = s2[level - 1, :, cols] + r2[level - 1, :, cols]
        exchange(c, level + 1).start()

    def close(c):
        cols = cols_of(c)
        last = bits - 1
        exchange(c, last).wait_recv()
        total = s2[last - 1, :, cols] + r2[last - 1, :, cols]
        out[bit, :, cols] = (tok[bit, :, cols].astype(jnp.float32) + total).astype(jnp.bfloat16)
        share(c).start()

    stages = [(0, multiply), (2, combine)]
    for level in range(1, bits - 1):
        stages.append((stages[-1][0] + 4, functools.partial(between, level=level)))
    stages.append((stages[-1][0] + 4, close))

    def tick(t, carry):
        for lag, stage in stages:
            @pl.when(jnp.logical_and(t >= lag, t < no + lag))
            def _(lag=lag, stage=stage):
                stage(t - lag)
        return carry

    lax.fori_loop(0, no + stages[-1][0], tick, 0)

    def drain(c, carry):
        halve(c).wait_send()
        for level in range(1, bits):
            exchange(c, level).wait_send()
        share(c).wait_send()
        shared(c).wait_recv()
        return carry

    lax.fori_loop(0, no, drain, 0)
    each(lambda d: spread(d).wait_send())
    each(lambda d: shift(nq, d, q_width, side).wait_send())
    for c in range(nq):
        each(lambda d: shift(c, d, c * q_chunk, q_chunk).wait_send())


def local(n, ny, tokens, lengths, norm_gain, w_query, key_value_weight, w_out, cache):
    batches, rows, depth = tokens.shape
    here = rows // n
    local_rows = batches * here
    q_width = w_query.shape[1]
    kv_heads = key_value_weight.shape[1]
    kv_width = kv_heads * key_value_weight.shape[2]
    assert kv_heads == 1 and ny >= 4 and ny & (ny - 1) == 0 and batches == 2
    heads = q_width // HEAD_SIZE
    out_width = w_out.shape[1]
    q_chunk = 512 if n <= 8 else q_width
    o_chunk = min(512, out_width)
    nq, no = q_width // q_chunk, out_width // o_chunk
    bits = ny.bit_length() - 1
    half = batches * rows // 2
    wide = q_width + kv_width + HEAD_SIZE
    freq = np.float32(ROPE_BASE) ** (
        -2.0 * np.arange(HEAD_SIZE // 2, dtype=np.float32) / HEAD_SIZE
    )
    freq = np.concatenate([freq, freq]).astype(np.float32)[None, :]
    pairs = cache.reshape(local_rows * cache.shape[2] * 2, HEAD_SIZE)
    any_space = pl.BlockSpec(memory_space=pl.ANY)
    f32, bf16 = jnp.float32, jnp.bfloat16
    dma = pltpu.SemaphoreType.DMA
    return pl.pallas_call(
        functools.partial(kernel, n, ny, q_chunk, o_chunk),
        out_shape=jax.ShapeDtypeStruct(tokens.shape, bf16),
        in_specs=[pl.BlockSpec(memory_space=pltpu.SMEM)] + [any_space] * 7,
        out_specs=pl.BlockSpec(memory_space=pltpu.VMEM),
        scratch_shapes=[
            pltpu.VMEM(tokens.shape, bf16),
            pltpu.VMEM((1, depth), f32),
            pltpu.VMEM((1, HEAD_SIZE), f32),
            pltpu.VMEM(w_query.shape, bf16),
            pltpu.VMEM((depth, kv_width), bf16),
            pltpu.VMEM(w_out.shape, bf16),
            pltpu.VMEM(pairs.shape, bf16),
            pltpu.VMEM((batches * rows, depth), bf16),
            pltpu.VMEM((n, local_rows, wide), f32),
            pltpu.VMEM((n, local_rows, wide), f32),
            pltpu.VMEM((local_rows, heads, HEAD_SIZE), f32),
            pltpu.VMEM((local_rows, heads, HEAD_SIZE), f32),
            pltpu.VMEM((local_rows, q_width), bf16),
            pltpu.VMEM((n, local_rows, q_width), bf16),
            pltpu.VMEM((batches * rows, q_width), f32),
            pltpu.VMEM((2, half, out_width), f32),
            pltpu.VMEM((half, out_width), f32),
            pltpu.VMEM((bits - 1, half, out_width), f32),
            pltpu.VMEM((bits - 1, half, out_width), f32),
            dma((3,)), dma((nq,)), dma, dma((no,)), dma,
            dma((nq + 1, n)), dma((nq + 1, n)), dma((n,)), dma((n,)),
            dma((no,)), dma((no,)), dma((bits - 1, no)), dma((bits - 1, no)),
            dma((no,)), dma((no,)),
        ],
        compiler_params=pltpu.CompilerParams(
            collective_id=0, has_side_effects=True, vmem_limit_bytes=60 * 1024 * 1024
        ),
    )(
        lengths, tokens, norm_gain.astype(f32).reshape(1, depth), jnp.asarray(freq),
        w_query, key_value_weight.reshape(depth, kv_width), w_out, pairs,
    )


def solution(mesh):
    placed = (
        P(None, "groups", "gx"),
        P(None, ("groups", "gx")),
        P("gx"),
        P("gx", "gy"),
        P("gx", "gy", None),
        P("gy", "gx"),
        P(None, ("groups", "gx"), None, "gy", None, None),
    )
    return jax.shard_map(
        functools.partial(local, mesh.shape["gx"], mesh.shape["gy"]),
        mesh=mesh, in_specs=placed, out_specs=P(None, "groups", "gx"), check_vma=False,
    )
```

```python
import functools

import jax
import jax.numpy as jnp
import numpy as np
from jax import lax
from jax.experimental import pallas as pl
from jax.experimental.pallas import tpu as pltpu
from jax.sharding import PartitionSpec as P

MODEL_WIDTH = 16384
HEAD_SIZE = 128
ROPE_BASE = 500000.0
MESH = pl.DeviceIdType.MESH


def kernel(
    n, ny, q_chunk, o_chunk,
    lens, tok_hbm, gain_hbm, freq_hbm, wq_hbm, wk_hbm, wo_hbm, kv_hbm,
    out,
    tok, gain, freq, wq, wk, wo, kv, normed,
    send, recv, q_s, o_s, att_send, att_recv, x_s, ybuf, r1, s2, r2,
    small_sem, wq_sem, wk_sem, wo_sem, kv_sem,
    qs_sem, qr_sem, as_sem, ar_sem, e_send, e_recv,
):
    batches, rows, depth = tok.shape
    here = rows // n
    total_rows = batches * rows
    q_width = wq.shape[1]
    kv_width = wk.shape[1]
    heads = q_width // HEAD_SIZE
    out_width = wo.shape[1]
    nq = q_width // q_chunk
    no = out_width // o_chunk
    local_rows = batches * here
    positions = kv.shape[0] // local_rows
    me = lax.axis_index("gx")
    my = lax.axis_index("gy")

    smalls = [
        pltpu.make_async_copy(tok_hbm, tok, small_sem.at[0]),
        pltpu.make_async_copy(gain_hbm, gain, small_sem.at[1]),
        pltpu.make_async_copy(freq_hbm, freq, small_sem.at[2]),
    ]
    for copy in smalls:
        copy.start()
    wk_copy = pltpu.make_async_copy(wk_hbm, wk, wk_sem)
    wk_copy.start()

    def wq_copy(c):
        cols = pl.ds(pl.multiple_of(c * q_chunk, q_chunk), q_chunk)
        return pltpu.make_async_copy(wq_hbm.at[:, cols], wq.at[:, cols], wq_sem.at[c])

    def wo_copy(c):
        cols = pl.ds(pl.multiple_of(c * o_chunk, o_chunk), o_chunk)
        return pltpu.make_async_copy(wo_hbm.at[:, cols], wo.at[:, cols], wo_sem.at[c])

    kv_copy = pltpu.make_async_copy(kv_hbm, kv, kv_sem)
    for c in range(nq):
        wq_copy(c).start()

    barrier = pltpu.get_barrier_semaphore()

    def greet(d, carry):
        pl.semaphore_signal(
            barrier, inc=1, device_id={"gx": lax.rem(me + d, n)}, device_id_type=MESH
        )
        return carry

    lax.fori_loop(1, n, greet, 0)
    bits = ny.bit_length() - 1

    def across(level):
        step = 1 << level
        return my + step - 2 * step * lax.rem(my // step, 2)

    for level in range(bits):
        pl.semaphore_signal(barrier, inc=1, device_id={"gy": across(level)}, device_id_type=MESH)

    for copy in smalls:
        copy.wait()
    x = tok[...].astype(jnp.float32).reshape(total_rows, depth)
    for k in range(depth // HEAD_SIZE):
        cols = slice(k * HEAD_SIZE, (k + 1) * HEAD_SIZE)
        normed[:, cols] = (x[:, cols] * gain[k:k + 1, :].astype(jnp.float32)).astype(jnp.bfloat16)
    squares = jnp.broadcast_to(jnp.sum(x * x, axis=1, keepdims=True), (total_rows, HEAD_SIZE))

    def put(part, start):
        width = part.shape[1]
        for j in range(n):
            for b in range(batches):
                send[j, b * here:(b + 1) * here, pl.ds(start, width)] = part[
                    b * rows + j * here:b * rows + (j + 1) * here, :
                ]

    def shift(c, d, start, width):
        target = lax.rem(me + d, n)
        cols = pl.ds(start, width)
        return pltpu.make_async_remote_copy(
            src_ref=send.at[target, :, cols],
            dst_ref=recv.at[me, :, cols],
            send_sem=qs_sem.at[c, d],
            recv_sem=qr_sem.at[c, d],
            device_id={"gx": target},
            device_id_type=MESH,
        )

    def arrive(c, d, start, width):
        source = lax.rem(me - d + n, n)
        cols = pl.ds(start, width)
        return pltpu.make_async_remote_copy(
            src_ref=send.at[source, :, cols],
            dst_ref=recv.at[source, :, cols],
            send_sem=qs_sem.at[c, d],
            recv_sem=qr_sem.at[c, d],
            device_id={"gx": source},
            device_id_type=MESH,
        )

    def each(fn):
        def body(d, carry):
            fn(d)
            return carry
        lax.fori_loop(1, n, body, 0)

    wk_copy.wait()
    xn = normed[...]
    put(jnp.dot(xn, wk[...], preferred_element_type=jnp.float32), q_width)
    put(squares, q_width + kv_width)
    pl.semaphore_wait(barrier, n - 1 + bits)
    side = kv_width + HEAD_SIZE
    each(lambda d: shift(nq, d, q_width, side).start())

    def project(c, carry):
        start = pl.multiple_of(c * q_chunk, q_chunk)
        wq_copy(c).wait()

        @pl.when(c == max(nq - 2, 0))
        def _():
            kv_copy.start()
            for o in range(no):
                wo_copy(o).start()

        put(
            jnp.dot(
                normed[...], wq[:, pl.ds(start, q_chunk)], preferred_element_type=jnp.float32
            ),
            start,
        )
        each(lambda d: shift(c, d, start, q_chunk).start())
        return carry

    lax.fori_loop(0, nq, project, 0)

    lane = lax.broadcasted_iota(jnp.int32, (local_rows, HEAD_SIZE), 1)
    row = lax.broadcasted_iota(jnp.int32, (local_rows, HEAD_SIZE), 0)
    place = jnp.zeros((local_rows, HEAD_SIZE), jnp.float32)
    for r in range(local_rows):
        place = jnp.where(row == r, lens[r // here, r % here].astype(jnp.float32), place)
    angle = place * freq[...]
    cosine = jnp.cos(angle)
    sine = jnp.sin(angle)
    sine = jnp.where(lane < HEAD_SIZE // 2, -sine, sine)

    def rotate(v):
        return v * cosine + pltpu.roll(v, HEAD_SIZE // 2, 1) * sine

    def finish(c, start, width):
        each(lambda d: arrive(c, d, start, width).wait_recv())

    def summed(start, width):
        cols = pl.ds(start, width)
        total = send[me, :, cols]

        def add(d, acc):
            return acc + recv[lax.rem(me + d, n), :, cols]

        return lax.fori_loop(1, n, add, total, unroll=n <= 8)

    finish(nq, q_width, side)
    tail = summed(q_width, side)
    scale = lax.rsqrt(tail[:, kv_width:] / MODEL_WIDTH + 1e-05)
    rkey = rotate(tail[:, :HEAD_SIZE] * scale)
    value_new = tail[:, HEAD_SIZE:2 * HEAD_SIZE] * scale

    for c in range(nq):
        finish(c, c * q_chunk, q_chunk)
        block = summed(c * q_chunk, q_chunk)
        for h in range(q_chunk // HEAD_SIZE):
            q_s[:, c * (q_chunk // HEAD_SIZE) + h, :] = rotate(
                block[:, h * HEAD_SIZE:(h + 1) * HEAD_SIZE] * scale
            )

    kv_copy.wait()
    inv_root = np.float32(1.0 / np.sqrt(np.float32(HEAD_SIZE)))
    column = lax.broadcasted_iota(jnp.int32, (heads, positions), 1)
    is_key = lax.rem(column, 2) == 0
    for r in range(local_rows):
        pairs = kv[r * positions:(r + 1) * positions, :]
        rquery = q_s[r].astype(jnp.bfloat16)
        scores = (
            lax.dot_general(
                rquery, pairs, (((1,), (1,)), ((), ())), preferred_element_type=jnp.float32
            )
            * inv_root
        )
        valid = jnp.logical_and(is_key, column < 2 * lens[r // here, r % here])
        scores = jnp.where(valid, scores, -1e30)
        new_score = (
            jnp.sum(rquery.astype(jnp.float32) * rkey[r:r + 1, :], axis=1, keepdims=True)
            * inv_root
        )
        top = jnp.maximum(jnp.max(scores, axis=1, keepdims=True), new_score)
        weights = jnp.exp(scores - top)
        new_weight = jnp.exp(new_score - top)
        total = jnp.sum(weights, axis=1, keepdims=True) + new_weight
        moved = pltpu.roll(weights, 1, 1).astype(jnp.bfloat16)
        mixed = jnp.dot(moved, pairs, preferred_element_type=jnp.float32)
        o_s[r] = (mixed + new_weight * value_new[r:r + 1, :]) / total

    for h in range(heads):
        att_send[:, h * HEAD_SIZE:(h + 1) * HEAD_SIZE] = o_s[:, h, :].astype(jnp.bfloat16)

    def spread(d):
        target = lax.rem(me + d, n)
        return pltpu.make_async_remote_copy(
            src_ref=att_send, dst_ref=att_recv.at[me],
            send_sem=as_sem.at[d], recv_sem=ar_sem.at[d],
            device_id={"gx": target}, device_id_type=MESH,
        )

    def gathered(d):
        source = lax.rem(me - d + n, n)
        return pltpu.make_async_remote_copy(
            src_ref=att_send, dst_ref=att_recv.at[source],
            send_sem=as_sem.at[d], recv_sem=ar_sem.at[d],
            device_id={"gx": source}, device_id_type=MESH,
        )

    each(lambda d: spread(d).start())
    att_recv[me] = att_send[...]
    each(lambda d: gathered(d).wait_recv())
    for j in range(n):
        block = att_recv[j].astype(jnp.float32)
        for b in range(batches):
            x_s[b * rows + j * here:b * rows + (j + 1) * here, :] = block[
                b * here:(b + 1) * here, :
            ]
    normed_att = x_s[...].astype(jnp.bfloat16)

    def cols_of(c):
        return pl.ds(pl.multiple_of(c * o_chunk, o_chunk), o_chunk)

    def exchange(c, k):
        cols = cols_of(c)
        return pltpu.make_async_remote_copy(
            src_ref=ybuf.at[:, cols] if k == 0 else s2.at[k - 1, :, cols],
            dst_ref=r1.at[:, cols] if k == 0 else r2.at[k - 1, :, cols],
            send_sem=e_send.at[k, c], recv_sem=e_recv.at[k, c],
            device_id={"gy": across(bits - 1 - k)}, device_id_type=MESH,
        )

    def multiply(c):
        cols = cols_of(c)
        wo_copy(c).wait()
        ybuf[:, cols] = jnp.dot(
            normed_att, wo[:, cols], preferred_element_type=jnp.float32
        ).astype(jnp.bfloat16)
        exchange(c, 0).start()

    def so_far(c, k):
        cols = cols_of(c)
        exchange(c, k).wait_recv()
        if k == 0:
            return ybuf[:, cols].astype(jnp.float32) + r1[:, cols].astype(jnp.float32)
        return s2[k - 1, :, cols] + r2[k - 1, :, cols]

    def combine(c, k):
        s2[k, :, cols_of(c)] = so_far(c, k)
        exchange(c, k + 1).start()

    def close(c):
        cols = cols_of(c)
        total = so_far(c, bits - 1).reshape(batches, rows, o_chunk)
        out[:, :, cols] = (tok[:, :, cols].astype(jnp.float32) + total).astype(jnp.bfloat16)

    stages = [(0, multiply)]
    for k in range(bits - 1):
        stages.append((stages[-1][0] + 3, functools.partial(combine, k=k)))
    stages.append((stages[-1][0] + 1, close))

    def tick(t, carry):
        for lag, stage in stages:
            @pl.when(jnp.logical_and(t >= lag, t < no + lag))
            def _(lag=lag, stage=stage):
                stage(t - lag)
        return carry

    lax.fori_loop(0, no + stages[-1][0], tick, 0)

    def drain(c, carry):
        for k in range(bits):
            exchange(c, k).wait_send()
        return carry

    lax.fori_loop(0, no, drain, 0)
    each(lambda d: spread(d).wait_send())
    each(lambda d: shift(nq, d, q_width, side).wait_send())
    for c in range(nq):
        each(lambda d: shift(c, d, c * q_chunk, q_chunk).wait_send())


def local(n, ny, tokens, lengths, norm_gain, w_query, key_value_weight, w_out, cache):
    batches, rows, depth = tokens.shape
    here = rows // n
    local_rows = batches * here
    q_width = w_query.shape[1]
    kv_heads = key_value_weight.shape[1]
    kv_width = kv_heads * key_value_weight.shape[2]
    assert kv_heads == 1 and ny >= 4 and ny & (ny - 1) == 0
    heads = q_width // HEAD_SIZE
    out_width = w_out.shape[1]
    q_chunk = 1024 if n <= 8 else q_width
    o_chunk = min(1024, out_width)
    nq, no = q_width // q_chunk, out_width // o_chunk
    bits = ny.bit_length() - 1
    wide = q_width + kv_width + HEAD_SIZE
    freq = np.float32(ROPE_BASE) ** (
        -2.0 * np.arange(HEAD_SIZE // 2, dtype=np.float32) / HEAD_SIZE
    )
    freq = np.concatenate([freq, freq]).astype(np.float32)[None, :]
    pairs = cache.reshape(local_rows * cache.shape[2] * 2, HEAD_SIZE)
    any_space = pl.BlockSpec(memory_space=pltpu.HBM)
    f32, bf16 = jnp.float32, jnp.bfloat16
    dma = pltpu.SemaphoreType.DMA
    return pl.pallas_call(
        functools.partial(kernel, n, ny, q_chunk, o_chunk),
        out_shape=pltpu.VMEM(tokens.shape, bf16),
        in_specs=[pl.BlockSpec(memory_space=pltpu.SMEM)] + [any_space] * 7,
        out_specs=pl.BlockSpec(memory_space=pltpu.VMEM),
        scratch_shapes=[
            pltpu.VMEM(tokens.shape, bf16),
            pltpu.VMEM((depth // HEAD_SIZE, HEAD_SIZE), bf16),
            pltpu.VMEM((1, HEAD_SIZE), f32),
            pltpu.VMEM(w_query.shape, bf16),
            pltpu.VMEM((depth, kv_width), bf16),
            pltpu.VMEM(w_out.shape, bf16),
            pltpu.VMEM(pairs.shape, bf16),
            pltpu.VMEM((batches * rows, depth), bf16),
            pltpu.VMEM((n, local_rows, wide), f32),
            pltpu.VMEM((n, local_rows, wide), f32),
            pltpu.VMEM((local_rows, heads, HEAD_SIZE), f32),
            pltpu.VMEM((local_rows, heads, HEAD_SIZE), f32),
            pltpu.VMEM((local_rows, q_width), bf16),
            pltpu.VMEM((n, local_rows, q_width), bf16),
            pltpu.VMEM((batches * rows, q_width), f32),
            pltpu.VMEM((batches * rows, out_width), bf16),
            pltpu.VMEM((batches * rows, out_width), bf16),
            pltpu.VMEM((bits - 1, batches * rows, out_width), f32),
            pltpu.VMEM((bits - 1, batches * rows, out_width), f32),
            dma((3,)), dma((nq,)), dma, dma((no,)), dma,
            dma((nq + 1, n)), dma((nq + 1, n)), dma((n,)), dma((n,)),
            dma((bits, no)), dma((bits, no)),
        ],
        compiler_params=pltpu.CompilerParams(
            collective_id=0, has_side_effects=True, vmem_limit_bytes=67043328 - 2 * tokens.size
        ),
    )(
        lengths, tokens, norm_gain.reshape(depth // HEAD_SIZE, HEAD_SIZE), jnp.asarray(freq),
        w_query, key_value_weight.reshape(depth, kv_width), w_out, pairs,
    )


def solution(mesh):
    placed = (
        P(None, "groups", "gx"),
        P(None, ("groups", "gx")),
        P("gx"),
        P("gx", "gy"),
        P("gx", "gy", None),
        P("gy", "gx"),
        P(None, ("groups", "gx"), None, "gy", None, None),
    )
    return jax.shard_map(
        functools.partial(local, mesh.shape["gx"], mesh.shape["gy"]),
        mesh=mesh, in_specs=placed, out_specs=P(None, "groups", "gx"), check_vma=False,
    )
```
